32 devices in a mesh: owner: 4 (over y, core), rows: 8 (over z, x).
Axes of the slice: x: 2, y: 2, z: 4, core: 2. Of those that a mesh axis runs over, the one named last changes fastest.
Arguments:
- w_down: float32 [16, 6400, 4096], P('owner', None, 'rows'), may hold values from -0.109375 to 0.109375
- avg_down: bfloat16 [16, 6400, 4096], P('owner', None, 'rows'), may hold values from -0.0390625 to 0.0390625
- router_weight: float32 [4096, 16], P('rows', 'owner'), may hold values from -0.09375 to 0.09375
- router_gain: float32 [4096], P('rows'), may hold values from 0.25 to 1.75
Outputs:
- serve_down: bfloat16 [16, 6400, 4096], P('owner', 'rows')
- scale_down: float32 [16, 6400], P('owner', 'rows')
- serve_router: bfloat16 [4096, 16], replicated
The draws below stay inside these ranges and needn't reach their ends.
All inputs are finite; a program needn't handle non-finite values.
Results may differ from the reference program's by a relative error of at most 0.0085.
Values may be sent and summed in bfloat16 or wider, within the bound.
A program may use at most 256 MiB of HBM per device.

```python
import jax
import jax.numpy as jnp
from jax import lax

EXPERTS = 16
D_MODEL = 4096
D_EXPERT = 6400


def spiked(drawn, rng, source, target, shards_of, factor):
    def block_of(dim):
        return (jnp.arange(drawn.shape[dim]) // (drawn.shape[dim] // shards_of)).reshape((-1,) + (1,) * (drawn.ndim - 1 - dim))

    one_side = jax.random.permutation(rng, shards_of)[block_of(target)]
    other_side = (block_of(target) + shards_of // 2) % shards_of
    return jnp.where((block_of(source) == one_side) | (block_of(source) == other_side), factor * drawn, drawn)


def block_scale(own_key, extent, cuts, smallest, high):
    factor_of = 1.0
    for position, shards_of in cuts:
        steps = jax.random.uniform(jax.random.fold_in(jax.random.fold_in(own_key, 6), position), (shards_of,), jnp.float32, smallest / len(cuts), high / len(cuts))
        factor_of = factor_of * jnp.repeat(jnp.exp(steps), extent[position] // shards_of).reshape((-1,) + (1,) * (len(extent) - 1 - position))
    return factor_of


def bell_draw(key, dims, width, most, pieces=(), dtype=jnp.bfloat16):
    values = width * jax.random.normal(key, dims, jnp.float32)
    if pieces:
        values = values * block_scale(key, dims, pieces, -0.22, 0.18)
    return jnp.clip(values, -most, most).astype(dtype)


def heavy_noise(key, dims, spread, reach, shards, heavy, dtype=jnp.bfloat16):
    array = spread * jax.random.normal(key, dims, jnp.float32)
    if shards:
        array = array * block_scale(key, dims, shards, -0.22, 0.18)
    return jnp.clip(spiked(array, jax.random.fold_in(key, 3), *heavy), -reach, reach).astype(dtype)


def setup_inputs(seed: int = 0) -> dict:
    seeds = jax.random.split(jax.random.key(seed), 5)
    return {
        "w_down": heavy_noise(seeds[0], (EXPERTS, D_EXPERT, D_MODEL), D_EXPERT ** -0.5, 0.109375, ((0, 4), (2, 8)), (2, 1, 8, 2.0), jnp.float32),
        "avg_down": bell_draw(seeds[1], (EXPERTS, D_EXPERT, D_MODEL), (D_EXPERT * 4) ** -0.5, 0.0390625, ((0, 4), (2, 8))),
        "router_weight": bell_draw(seeds[2], (D_MODEL, EXPERTS), D_MODEL ** -0.5, 0.09375, ((0, 8), (1, 4)), jnp.float32),
        "router_gain": jnp.clip(1.0 + 0.15 * jax.random.normal(seeds[3], (D_MODEL,), jnp.float32), 0.25, 1.75),
    }


def reference(w_down, avg_down, router_weight, router_gain):
    fresh_down = w_down + avg_down.astype(jnp.float32)
    scale_down = jnp.sqrt(lax.optimization_barrier(jnp.sum(fresh_down * fresh_down, axis=2)))
    serve_down = (fresh_down / jnp.expand_dims(scale_down, 2)).astype(jnp.bfloat16)
    serve_router = (router_weight * router_gain[:, None]).astype(jnp.bfloat16)
    return (serve_down, scale_down, serve_router)
```

```python
import functools
import math

import jax
import jax.numpy as jnp
from jax import lax
from jax.experimental import pallas as pl
from jax.experimental.pallas import tpu as pltpu
from jax.sharding import PartitionSpec as P

MESH = pl.DeviceIdType.MESH
ANY = pl.ANY
TAIL_SHARE = 13


def divisor(size, most, step):
    for d in range(min(size, most) // step * step, 0, -step):
        if size % d == 0:
            return d
    return size


def receiver(n, me, t):
    if n % 4:
        return lax.rem(me + 1 + t, n)
    half = n // 2
    side, place = me // half, lax.rem(me, half)
    middle = lax.rem((me + n // 4) // half, 2)
    u = lax.rem(t + (1 - middle) * half, n - 1)
    across = u // half
    i = u - across * (half - 1)
    to_side = (1 - side) * (1 - across) + side * across
    return to_side * half + lax.rem(place + i, half)


def exchange_body(n, keep, w, a, r, got, tail, gotr, wbuf, abuf, packed, in_sem, send_sem, recv_sem, own_sem, tail_sem, r_sem):
    experts, _, per, cols = w.shape
    me = lax.axis_index("rows")
    block = divisor(per, 80, 8)
    rows_of = [per] * (experts - 1) + [per - keep]

    def dest(t):
        return jnp.where(t == n - 1, me, receiver(n, me, jnp.minimum(t, n - 2)))

    def loads(t, e):
        d = dest(t)
        return (
            pltpu.make_async_copy(w.at[e, d], wbuf.at[e], in_sem.at[0, e]),
            pltpu.make_async_copy(a.at[e, d], abuf.at[e], in_sem.at[1, e]),
        )

    def remote(src_dev, to, e):
        rows = pl.ds(e * per, rows_of[e])
        return pltpu.make_async_remote_copy(
            src_ref=packed.at[to, rows],
            dst_ref=got.at[src_dev, rows],
            send_sem=send_sem.at[to, e],
            recv_sem=recv_sem.at[src_dev, e],
            device_id={"rows": to},
            device_id_type=MESH,
        )

    def own(e):
        rows = pl.ds(e * per, rows_of[e])
        return pltpu.make_async_copy(packed.at[me, rows], got.at[me, rows], own_sem.at[e])

    def tail_copy(d):
        rows = pl.ds(experts * per - keep, keep)
        return pltpu.make_async_copy(packed.at[d, rows], tail.at[d], tail_sem.at[d])

    def r_remote(src_dev, to):
        return pltpu.make_async_remote_copy(
            src_ref=r,
            dst_ref=gotr.at[src_dev],
            send_sem=r_sem.at[0, to],
            recv_sem=r_sem.at[1, src_dev],
            device_id={"rows": to},
            device_id_type=MESH,
        )

    def r_own():
        return pltpu.make_async_copy(r, gotr.at[me], r_sem.at[0, me])

    for e in range(experts):
        for copy in loads(0, e):
            copy.start()
    barrier = pltpu.get_barrier_semaphore()

    @pl.loop(1, n)
    def _(i):
        pl.semaphore_signal(barrier, inc=1, device_id={"rows": lax.rem(me + i, n)}, device_id_type=MESH)

    pl.semaphore_wait(barrier, n - 1)
    r_own().start()

    def send(t, e):
        @pl.when(t < n - 1)
        def _():
            remote(me, dest(t), e).start()

        @pl.when(t == n - 1)
        def _():
            own(e).start()

        if e == experts - 1:
            tail_copy(dest(t)).start()

    @pl.loop(0, n)
    def _(t):
        d = dest(t)
        for e in range(experts):
            for copy in loads(t, e):
                copy.wait()
            if e:
                send(t, e - 1)
            else:

                @pl.when(t > 0)
                def _():
                    send(t - 1, experts - 1)

            @pl.loop(0, per // block)
            def _(b):
                rows = pl.ds(pl.multiple_of(b * block, block), block)
                into = pl.ds(pl.multiple_of(e * per + b * block, math.gcd(block, per)), block)
                packed[d, into] = (wbuf[e, rows] + abuf[e, rows].astype(jnp.float32)).astype(packed.dtype)

            @pl.when(t < n - 1)
            def _():
                for copy in loads(t + 1, e):
                    copy.start()

    send(n - 1, experts - 1)

    @pl.loop(1, n)
    def _(i):
        r_remote(me, lax.rem(me + i, n)).start()

    @pl.loop(1, n)
    def _(i):
        other = lax.rem(me + i, n)
        for e in range(experts):
            remote(me, other, e).wait_send()
            remote(other, me, e).wait_recv()
        r_remote(me, other).wait_send()
        r_remote(other, me).wait_recv()
        tail_copy(other).wait()

    for e in range(experts):
        own(e).wait()
    tail_copy(me).wait()
    r_own().wait()


def exchange(n, keep, w, a, r):
    experts, _, per, cols = w.shape
    any_spec = pl.BlockSpec(memory_space=ANY)
    bf16 = jnp.bfloat16
    return pl.pallas_call(
        functools.partial(exchange_body, n, keep),
        in_specs=[any_spec] * 3,
        out_specs=[any_spec] * 3,
        out_shape=[
            jax.ShapeDtypeStruct((n, experts * per - keep, cols), bf16),
            jax.ShapeDtypeStruct((n, keep, cols), bf16),
            jax.ShapeDtypeStruct((n,) + r.shape, bf16),
        ],
        scratch_shapes=[
            pltpu.VMEM((experts, per, cols), jnp.float32),
            pltpu.VMEM((experts, per, cols), bf16),
            pltpu.VMEM((n, experts * per, cols), bf16),
            pltpu.SemaphoreType.DMA((2, experts)),
            pltpu.SemaphoreType.DMA((n, experts)),
            pltpu.SemaphoreType.DMA((n, experts)),
            pltpu.SemaphoreType.DMA((experts,)),
            pltpu.SemaphoreType.DMA((n,)),
            pltpu.SemaphoreType.DMA((2, n)),
        ],
        compiler_params=pltpu.CompilerParams(
            collective_id=0, has_side_effects=True, vmem_limit_bytes=63 * 2**20
        ),
        name="exchange",
    )(w, a, r)


def norm_body(n, cols, got, *rest):
    serve, scale = rest[-2:]
    total = None
    for s in range(n):
        x = got[s].astype(jnp.float32)
        part = jnp.sum(x * x, axis=1, keepdims=True)
        total = part if total is None else total + part
    root = jnp.sqrt(total)
    inverse = 1.0 / root
    for s in range(n):
        x = got[s].astype(jnp.float32)
        serve[:, s * cols : (s + 1) * cols] = (x * inverse).astype(serve.dtype)
    scale[...] = jnp.broadcast_to(root, scale.shape)


def norm(got, serve, first, count, rb):
    n, here, cols = got.shape
    specs, args, alias = [pl.BlockSpec((n, rb, cols), lambda i: (0, i, 0))], [got], {}
    if serve is not None:
        specs.append(pl.BlockSpec(memory_space=ANY))
        args.append(serve)
        alias = {1: 0}
    return pl.pallas_call(
        functools.partial(norm_body, n, cols),
        grid=(here // rb,),
        in_specs=specs,
        out_specs=[
            pl.BlockSpec((rb, n * cols), lambda i: (first // rb + i, 0)),
            pl.BlockSpec((rb, 128), lambda i: (i, 0)),
        ],
        out_shape=[
            jax.ShapeDtypeStruct((count, n * cols), jnp.bfloat16),
            jax.ShapeDtypeStruct((here, 128), jnp.float32),
        ],
        input_output_aliases=alias,
        cost_estimate=pl.CostEstimate(
            flops=6 * n * here * cols, bytes_accessed=4 * n * here * cols, transcendentals=0
        ),
        name="norm",
    )(*args)


def local(n, w_down, avg_down, router_weight, router_gain):
    experts, rows, cols = w_down.shape
    per = rows // n
    mine = router_weight.shape[1]
    keep = per % 16 + 16 * max(1, -(-experts * per // TAIL_SHARE) // 16)
    keep = min(keep, per)
    count = experts * per
    rb = divisor(math.gcd(count - keep, keep), 80, 8)
    part = (router_weight * router_gain[:, None]).astype(jnp.bfloat16).T
    part = jnp.pad(part, ((0, -mine % 16), (0, 0)))
    got, tail, gotr = exchange(
        n, keep, w_down.reshape(experts, n, per, cols), avg_down.reshape(experts, n, per, cols), part
    )
    last = lax.all_to_all(tail, "rows", split_axis=0, concat_axis=0, tiled=True)
    rows_of = gotr[:, :mine, :].transpose(1, 0, 2).reshape(mine, n * cols)
    router = lax.all_gather(rows_of, "owner", axis=0, tiled=True).T
    serve, scale = norm(got, None, 0, count, rb)
    scale = scale[:, 0]
    serve, scale, last, router = lax.optimization_barrier((serve, scale, last, router))
    serve, scale_last = norm(last, serve, count - keep, count, rb)
    scale = jnp.concatenate([scale, scale_last[:, 0]]).reshape(experts, per)
    return serve.reshape(experts, per, n * cols), scale, router


def solution(mesh):
    return jax.shard_map(
        functools.partial(local, mesh.shape["rows"]),
        mesh=mesh,
        in_specs=(
            P("owner", None, "rows"),
            P("owner", None, "rows"),
            P("rows", "owner"),
            P("rows"),
        ),
        out_specs=(P("owner", "rows", None), P("owner", "rows"), P()),
        check_vma=False,
    )
```
